256 devices in a mesh: tok: 32 (over z_lo, x, core), blk: 8 (over y, z_hi).
Axes of the slice: x: 4, y: 4, z: 8 (z_hi: 2, z_lo: 4; z = z_hi * 4 + z_lo), core: 2. Of those that a mesh axis runs over, the one named last changes fastest.
Arguments:
- activations: bfloat16 [4096, 7168], P('tok', 'blk'), may hold values from -600 to 600
- signs: float32 [7168], P('blk'), may hold values from -1 to 1, as said below
Outputs:
- hessian: float32 [7168, 7168], P('tok', 'blk')
- incoherence: float32 [7168], P('blk')
- largest_ratio: float32 [], replicated
The draws below stay inside these ranges and needn't reach their ends.
Inputs may be any that keep to these rules, and one draw needn't show every extreme that they name: `signs`: every entry is -1 or 1.
All inputs are finite; a program needn't handle non-finite values.
Results may differ from the reference program's by a relative error of at most 0.0037.
Values may be sent and summed in bfloat16 or wider, within the bound.
A program may use at most 128 MiB of HBM per device.

```python
import math
import jax
import jax.numpy as jnp
from jax import lax

WALSH = 512
MIX = 14
FEATURES = 7168
TOKENS = 4096


def draw_activations(key, part):
    noise_key, scale_key = jax.random.split(key, 2)
    position = jnp.arange(TOKENS, dtype=jnp.float32) / TOKENS
    ramp = jnp.exp(math.log(3.0) * position)[:, None]
    row_scale = jnp.exp(jax.random.uniform(scale_key, (TOKENS, 1), jnp.float32, 0.0, math.log(10.0)))
    values = jnp.clip(jax.random.normal(noise_key, (TOKENS, FEATURES), jnp.float32), -5.0, 5.0)
    return (values * ramp * row_scale).astype(jnp.bfloat16)


def draw_signs(key, part):
    coins = jax.random.randint(key, (FEATURES,), 0, 2)
    return (2 * coins - 1).astype(jnp.float32)


def setup_inputs(seed: int = 0) -> dict:
    seeds = jax.random.split(jax.random.key(seed), 3)
    return {
        "activations": draw_activations(jax.random.fold_in(seeds[2], 71), 0),
        "signs": draw_signs(jax.random.fold_in(seeds[2], 71), 0),
    }


EPS = 1e-06
DAMP = 0.01

def walsh_table(length):
    position = jnp.arange(length, dtype=jnp.int32)
    parity = jnp.zeros((length, length), jnp.int32)
    for bit_number in range(length.bit_length() - 1):
        parity = parity + (position[:, None] >> bit_number & 1) * (position[None, :] >> bit_number & 1)
    return (1 - 2 * (parity % 2)).astype(jnp.float32)

def cosine_table(length):
    rows_idx = jnp.arange(length, dtype=jnp.float32)[:, None]
    columns = jnp.arange(length, dtype=jnp.float32)[None, :]
    table = math.sqrt(2.0 / length) * jnp.cos(math.pi * (columns + 0.5) * rows_idx / length)
    return jnp.where(rows_idx == 0.0, table * math.sqrt(0.5), table)

def reference(activations, signs):
    signed = activations * signs.astype(jnp.bfloat16)[None, :]
    tokens_total = activations.shape[0]
    values = signed.astype(jnp.float32).reshape(tokens_total, WALSH, MIX)
    values = jnp.einsum('tba,ka->tbk', values, cosine_table(MIX), precision=lax.Precision.HIGHEST)
    values = jnp.einsum('tbk,cb->tck', values, walsh_table(WALSH) / math.sqrt(WALSH), precision=lax.Precision.HIGHEST)
    rotated = values.reshape(tokens_total, FEATURES).astype(jnp.bfloat16)
    gram_matrix = lax.dot_general(rotated, rotated, (((0,), (0,)), ((), ())), preferred_element_type=jnp.float32)
    on_diag = jnp.eye(FEATURES, dtype=jnp.bool_)
    trace_total = jnp.sum(jnp.diagonal(gram_matrix))
    diag_mean = trace_total / FEATURES + EPS
    hessian = gram_matrix / diag_mean + DAMP * on_diag.astype(jnp.float32)
    column_peak = lax.optimization_barrier(jnp.max(jnp.where(on_diag, 0.0, jnp.abs(gram_matrix)), axis=0))
    incoherence = column_peak / diag_mean
    return (hessian, incoherence, jnp.max(incoherence))
```

```python
import math

import jax
import jax.numpy as jnp
import numpy as np
from jax import lax
from jax.sharding import PartitionSpec as P

WALSH = 512
MIX = 14
FEATURES = 7168
EPS = 1e-06
DAMP = 0.01


def walsh(length):
    table = np.ones((1, 1))
    while table.shape[0] < length:
        table = np.block([[table, table], [table, -table]])
    return table


def cosine(length):
    k = np.arange(length)[:, None]
    n = np.arange(length)[None, :]
    table = math.sqrt(2.0 / length) * np.cos(math.pi * (n + 0.5) * k / length)
    table[0] *= math.sqrt(0.5)
    return table


def split_table(local):
    table = np.kron(walsh(local), cosine(MIX).T) / math.sqrt(WALSH)
    high = table.astype(jnp.bfloat16)
    low = (table - high.astype(np.float64)).astype(jnp.bfloat16)
    return high, low


def contract_tokens(left, right):
    return lax.dot_general(left, right, (((0,), (0,)), ((), ())), preferred_element_type=jnp.float32)


def combine(parts):
    parts = list(parts)
    step = 1
    while step < len(parts):
        for i in range(0, len(parts), 2 * step):
            for j in range(i, i + step):
                parts[j], parts[j + step] = parts[j] + parts[j + step], parts[j] - parts[j + step]
        step *= 2
    return parts


def per_device(activations, signs):
    rows, width = activations.shape
    blocks = lax.axis_size("blk")
    toks = lax.axis_size("tok")
    b = lax.axis_index("blk")
    t = lax.axis_index("tok")
    share = rows // blocks
    row_count = FEATURES // toks
    high, low = split_table(WALSH // blocks)
    signed = activations * signs.astype(jnp.bfloat16)[None, :]
    mine = lax.all_to_all(signed.reshape(blocks, share, width), "blk", 0, 0, tiled=True)
    flat = mine.reshape(blocks * share, width)
    mixed = jnp.dot(flat, high, preferred_element_type=jnp.float32)
    mixed = mixed + jnp.dot(flat, low, preferred_element_type=jnp.float32)
    mixed = mixed.reshape(blocks, share, width)
    rotated = jnp.stack(combine([mixed[i] for i in range(blocks)])).astype(jnp.bfloat16)
    wide = rotated.astype(jnp.float32)
    trace_total = lax.psum(jnp.sum(wide * wide), ("tok", "blk"))
    columns = lax.all_to_all(rotated, "blk", 0, 0, tiled=True).reshape(rows, width)
    columns = lax.all_gather(columns, "tok", axis=0, tiled=True)
    pieces = jnp.moveaxis(rotated, 0, 1).reshape(share, toks, row_count)
    pieces = lax.all_to_all(jnp.moveaxis(pieces, 1, 0), "tok", 0, 0, tiled=True)
    pieces = lax.all_gather(pieces, "blk", axis=1, tiled=False)
    left = pieces.reshape(toks * rows, row_count)
    gram = contract_tokens(left, columns)
    at_rows = t * row_count + jnp.arange(row_count, dtype=jnp.int32)[:, None]
    at_columns = b * width + jnp.arange(width, dtype=jnp.int32)[None, :]
    on_diag = at_rows == at_columns
    peaks = jnp.max(jnp.where(on_diag, 0.0, jnp.abs(gram)), axis=0)
    peak = lax.pmax(peaks, "tok")
    largest = lax.pmax(jnp.max(peak), "blk")
    diag_mean = trace_total / FEATURES + EPS
    hessian = gram / diag_mean + DAMP * on_diag.astype(jnp.float32)
    return hessian, peak / diag_mean, largest / diag_mean


def solution(mesh):
    return jax.shard_map(
        per_device,
        mesh=mesh,
        in_specs=(P("tok", "blk"), P("blk")),
        out_specs=(P("tok", "blk"), P("blk"), P()),
        check_vma=False,
    )
```
